8 devices in a mesh: batch: 1 (over z), col: 2 (over y), row: 4 (over x, core).
Axes of the slice: x: 2, y: 2, z: 1, core: 2. Of those that a mesh axis runs over, the one named last changes fastest.
Arguments:
- d_inv: bfloat16 [24, 1024, 1024], P(('batch', 'row'))
- l_blk: bfloat16 [24, 1024, 1024], P(('batch', 'row'))
- u_blk: bfloat16 [24, 1024, 1024], P(('batch', 'row'))
- rhs_blk: float32 [24, 1024, 256], P(('batch', 'row'), None, 'col')
- x_init: float32 [24, 1024, 256], P(('batch', 'row'), None, 'col')
Outputs:
- output: float32 [24, 1024, 256], P(('batch', 'row'), None, 'col')
All inputs are finite; a program needn't handle non-finite values.
Results may differ from the reference program's by a relative error of at most 0.0111632.
Values are sent between devices in bfloat16 or wider.
A program may use at most 1 GiB of HBM per device.

```python
import jax
import jax.numpy as jnp
from jax import lax

BLOCK_ROWS = 24
BLOCK_SIZE = 1024
RHS_COLS = 256
SWEEPS = 4


def setup_inputs(seed: int = 0, part: int = 0) -> dict:
    base_key = jax.random.fold_in(jax.random.key(seed), part)
    k_d, k_l, k_u, k_f, k_x = jax.random.split(base_key, 5)
    fan_scale = BLOCK_SIZE ** -0.5
    mat_shape = (BLOCK_ROWS, BLOCK_SIZE, BLOCK_SIZE)
    vec_shape = (BLOCK_ROWS, BLOCK_SIZE, RHS_COLS)
    ident_mat = jnp.eye(BLOCK_SIZE, dtype=jnp.float32)
    row_ids = jnp.arange(BLOCK_ROWS)
    l_mask = (row_ids > 0).astype(jnp.float32)[:, None, None]
    u_mask = (row_ids < BLOCK_ROWS - 1).astype(jnp.float32)[:, None, None]
    d_inv = ident_mat + 0.3 * fan_scale * jax.random.normal(k_d, mat_shape, jnp.float32)
    l_blk = 0.6 * fan_scale * jax.random.normal(k_l, mat_shape, jnp.float32) * l_mask
    u_blk = 0.45 * fan_scale * jax.random.normal(k_u, mat_shape, jnp.float32) * u_mask
    rhs_blk = jax.random.normal(k_f, vec_shape, jnp.float32)
    x_init = jax.random.normal(k_x, vec_shape, jnp.float32)
    return {"d_inv": d_inv.astype(jnp.bfloat16), "l_blk": l_blk.astype(jnp.bfloat16), "u_blk": u_blk.astype(jnp.bfloat16), "rhs_blk": rhs_blk, "x_init": x_init}


def reference(d_inv, l_blk, u_blk, rhs_blk, x_init):
    zero_blk = jnp.zeros((BLOCK_SIZE, RHS_COLS), jnp.float32)

    def row_step(x_left, row_in):
        d_i, l_i, u_i, f_i, x_right = row_in
        t_i = (f_i
               - jnp.dot(l_i, x_left.astype(jnp.bfloat16), preferred_element_type=jnp.float32)
               - jnp.dot(u_i, x_right.astype(jnp.bfloat16), preferred_element_type=jnp.float32))
        x_i = jnp.dot(d_i, t_i.astype(jnp.bfloat16), preferred_element_type=jnp.float32)
        return x_i, x_i

    def one_sweep(x_old, unused):
        x_right = jnp.concatenate([x_old[1:], zero_blk[None]], axis=0)
        _, x_new = lax.scan(row_step, zero_blk, (d_inv, l_blk, u_blk, rhs_blk, x_right))
        return x_new, None

    x_final, _ = lax.scan(one_sweep, x_init, None, length=SWEEPS)
    return x_final
```

```python
import jax
import jax.numpy as jnp
from jax import lax
from jax.experimental import pallas as pl
from jax.experimental.pallas import tpu as pltpu
from jax.sharding import PartitionSpec as P

SWEEPS = 4
TILE = 256
U, L, D = 0, 1, 2


def kernel(chain_len, d_hbm, l_hbm, u_hbm, f_hbm, x_hbm, o_hbm,
           w, nat, xraw, ft, xt, rl, rr,
           w_sem, f_sem, x_sem, o_sem, fs_sem, fr_sem, bs_sem, br_sem):
    pos = lax.axis_index("row")
    rows, size, _ = d_hbm.shape
    tiles = size // TILE
    has_left, has_right = pos > 0, pos < chain_len - 1
    hbm = {U: u_hbm, L: l_hbm, D: d_hbm}

    def w_copy(kind, row):
        slot = kind * rows + row
        return pltpu.make_async_copy(hbm[kind].at[row], w.at[slot], w_sem.at[slot])

    def f_copy(row):
        return pltpu.make_async_copy(f_hbm.at[row], nat.at[row], f_sem.at[row])

    def x_copy(row):
        return pltpu.make_async_copy(x_hbm.at[row], xraw.at[row], x_sem.at[row])

    def o_copy(row):
        return pltpu.make_async_copy(nat.at[row], o_hbm.at[row], o_sem.at[row])

    def fwd_copy(k):
        return pltpu.make_async_remote_copy(
            src_ref=xt.at[rows - 1], dst_ref=rl.at[k], send_sem=fs_sem.at[k], recv_sem=fr_sem.at[k],
            device_id={"row": pos + 1}, device_id_type=pl.DeviceIdType.MESH)

    def back_copy(k):
        return pltpu.make_async_remote_copy(
            src_ref=xt.at[0], dst_ref=rr.at[k], send_sem=bs_sem.at[k], recv_sem=br_sem.at[k],
            device_id={"row": pos - 1}, device_id_type=pl.DeviceIdType.MESH)

    x_copy(0).start()
    for row in range(rows):
        if row + 1 < rows:
            x_copy(row + 1).start()
        f_copy(row).start()
        w_copy(U, row).start()
        if row > 0:
            w_copy(L, row).start()
        w_copy(D, row).start()
    w_copy(L, 0).start()

    barrier = pltpu.get_barrier_semaphore()

    @pl.when(has_left)
    def _():
        pl.semaphore_signal(barrier, inc=1, device_id={"row": pos - 1}, device_id_type=pl.DeviceIdType.MESH)

    @pl.when(has_right)
    def _():
        pl.semaphore_signal(barrier, inc=1, device_id={"row": pos + 1}, device_id_type=pl.DeviceIdType.MESH)

    pl.semaphore_wait(barrier, has_left.astype(jnp.int32) + has_right.astype(jnp.int32))

    def transpose_w(slot):
        for a in range(tiles):
            for b in range(a, tiles):
                ra, rb = pl.ds(a * TILE, TILE), pl.ds(b * TILE, TILE)
                upper = w[slot, ra, rb]
                if a == b:
                    w[slot, ra, rb] = upper.T
                else:
                    lower = w[slot, rb, ra]
                    w[slot, ra, rb] = lower.T
                    w[slot, rb, ra] = upper.T

    x_copy(0).wait()
    xt[0] = xraw[0].T.astype(jnp.bfloat16)

    @pl.when(has_left)
    def _():
        back_copy(0).start()

    @pl.when(jnp.logical_not(has_left))
    def _():
        for k in range(SWEEPS):
            rl[k] = jnp.zeros(rl.shape[1:], rl.dtype)

    @pl.when(jnp.logical_not(has_right))
    def _():
        for k in range(SWEEPS):
            rr[k] = jnp.zeros(rr.shape[1:], rr.dtype)

    def prep(row, kind):
        pltpu.make_async_copy(hbm[kind].at[row], w.at[kind * rows + row], w_sem.at[kind * rows + row]).wait()
        transpose_w(kind * rows + row)

    def prep_row(row, carry):
        f_copy(row).wait()
        ft[row] = nat[row].T

        @pl.when(row > 0)
        def _():
            x_copy(row).wait()
            xt[row] = xraw[row].T.astype(jnp.bfloat16)

        prep(row, U)
        prep(row, L)
        prep(row, D)
        return carry

    lax.fori_loop(0, rows, prep_row, 0)

    def product(x, slot):
        return jnp.dot(x, w[slot], preferred_element_type=jnp.float32)

    def sweep(k, last):
        for row in range(rows):
            if row == rows - 1:
                @pl.when(has_right)
                def _():
                    back_copy(k).wait_recv()
            right = rr[k] if row == rows - 1 else xt[row + 1]
            t = ft[row] - product(right, U * rows + row)
            if row == 0:
                @pl.when(has_left)
                def _():
                    fwd_copy(k).wait_recv()
            left = rl[k] if row == 0 else xt[row - 1]
            t = t - product(left, L * rows + row)
            x_new = product(t.astype(jnp.bfloat16), D * rows + row)
            if row == 0:
                @pl.when(has_left)
                def _():
                    back_copy(k).wait_send()
            if row == rows - 1 and not (isinstance(k, int) and k == 0):
                @pl.when(has_right & (k > 0))
                def _():
                    fwd_copy(k - 1).wait_send()
            xt[row] = x_new.astype(jnp.bfloat16)
            if row == 0 and not last:
                @pl.when(has_left)
                def _():
                    back_copy(k + 1).start()
            if row == rows - 1:
                @pl.when(has_right)
                def _():
                    fwd_copy(k).start()
            if last:
                nat[row] = x_new.T
                o_copy(row).start()

    def mid_sweep(k, carry):
        sweep(k, False)
        return carry

    lax.fori_loop(0, SWEEPS - 1, mid_sweep, 0)
    sweep(SWEEPS - 1, True)

    @pl.when(has_right)
    def _():
        fwd_copy(SWEEPS - 1).wait_send()

    for row in range(rows):
        o_copy(row).wait()


def solution(mesh):
    chain_len = mesh.shape["row"]
    mat_spec = P(("batch", "row"), None, None)
    vec_spec = P(("batch", "row"), None, "col")

    def device_fn(d_inv, l_blk, u_blk, rhs_blk, x_init):
        rows, size, cols = rhs_blk.shape
        any_spec = pl.BlockSpec(memory_space=pl.ANY)
        dma = pltpu.SemaphoreType.DMA
        return pl.pallas_call(
            lambda *refs: kernel(chain_len, *refs),
            out_shape=jax.ShapeDtypeStruct(rhs_blk.shape, jnp.float32),
            in_specs=[any_spec] * 5,
            out_specs=any_spec,
            scratch_shapes=[
                pltpu.VMEM((3 * rows, size, size), jnp.bfloat16),
                pltpu.VMEM((rows, size, cols), jnp.float32),
                pltpu.VMEM((rows, size, cols), jnp.float32),
                pltpu.VMEM((rows, cols, size), jnp.float32),
                pltpu.VMEM((rows, cols, size), jnp.bfloat16),
                pltpu.VMEM((SWEEPS, cols, size), jnp.bfloat16),
                pltpu.VMEM((SWEEPS, cols, size), jnp.bfloat16),
                dma((3 * rows,)), dma((rows,)), dma((rows,)), dma((rows,)),
                dma((SWEEPS,)), dma((SWEEPS,)), dma((SWEEPS,)), dma((SWEEPS,)),
            ],
            compiler_params=pltpu.CompilerParams(
                collective_id=0, has_side_effects=True, vmem_limit_bytes=60 * 1024 * 1024),
        )(d_inv, l_blk, u_blk, rhs_blk, x_init)

    return jax.shard_map(device_fn, mesh=mesh, in_specs=(mat_spec, mat_spec, mat_spec, vec_spec, vec_spec),
                         out_specs=vec_spec, check_vma=False)
```

```python
import jax
import jax.numpy as jnp
from jax import lax
from jax.experimental import pallas as pl
from jax.experimental.pallas import tpu as pltpu
from jax.sharding import PartitionSpec as P

SWEEPS = 4
TILE = 256
GROUPS = 2
MESH = pl.DeviceIdType.MESH
F32, BF16 = jnp.float32, jnp.bfloat16


def kernel(chain_len, d_hbm, l_hbm, u_hbm, f_hbm, x_hbm, out,
           wu, wl, wd, fraw, xraw, ft, st, tmp, tb, xt, rl, rr,
           u_sem, l_sem, d_sem, f_sem, x_sem, fs_sem, fr_sem, bs_sem, br_sem):
    pos = lax.axis_index("row")
    rows, size, _ = d_hbm.shape
    cols = xt.shape[1]
    gcols = cols // GROUPS
    tiles = size // TILE
    first, has_left, has_right = pos == 0, pos > 0, pos < chain_len - 1
    mid = chain_len // 2
    last_row = rows - 1
    everything = pl.ds(0, cols)

    def u_copy(row):
        return pltpu.make_async_copy(u_hbm.at[row], wu.at[row], u_sem.at[row])

    def l_copy(row):
        return pltpu.make_async_copy(l_hbm.at[row], wl.at[row], l_sem.at[row])

    def d_copy(row):
        return pltpu.make_async_copy(d_hbm.at[row], wd.at[row], d_sem.at[row])

    def f_copy(row):
        return pltpu.make_async_copy(f_hbm.at[row], fraw.at[row], f_sem.at[row])

    def x_copy(row):
        return pltpu.make_async_copy(x_hbm.at[row], xraw.at[row], x_sem.at[row])

    def group(g):
        return pl.ds(g * gcols, gcols)

    def fwd_copy(k, g):
        return pltpu.make_async_remote_copy(
            src_ref=xt.at[last_row, group(g)], dst_ref=rl.at[k, group(g)],
            send_sem=fs_sem.at[k, g], recv_sem=fr_sem.at[k, g],
            device_id={"row": pos + 1}, device_id_type=MESH)

    def back_copy(k, g):
        return pltpu.make_async_remote_copy(
            src_ref=xt.at[0, group(g)], dst_ref=rr.at[k, group(g)],
            send_sem=bs_sem.at[k, g], recv_sem=br_sem.at[k, g],
            device_id={"row": pos - 1}, device_id_type=MESH)

    def load_u(row):
        f_copy(row).start()
        if isinstance(row, int):
            if row + 1 < rows:
                x_copy(row + 1).start()
        else:
            @pl.when(row + 1 < rows)
            def _():
                x_copy(row + 1).start()
        u_copy(row).start()

    x_copy(0).start()
    load_u(0)
    d_copy(0).start()
    load_u(1)
    l_copy(1).start()

    barrier = pltpu.get_barrier_semaphore()

    @pl.when(has_left)
    def _():
        pl.semaphore_signal(barrier, inc=1, device_id={"row": pos - 1}, device_id_type=MESH)

    @pl.when(has_right)
    def _():
        pl.semaphore_signal(barrier, inc=1, device_id={"row": pos + 1}, device_id_type=MESH)

    pl.semaphore_wait(barrier, has_left.astype(jnp.int32) + has_right.astype(jnp.int32))

    @pl.when(jnp.logical_not(has_left))
    def _():
        for k in range(SWEEPS):
            rl[k] = jnp.zeros(rl.shape[1:], rl.dtype)

    @pl.when(jnp.logical_not(has_right))
    def _():
        for k in range(SWEEPS):
            rr[k] = jnp.zeros(rr.shape[1:], rr.dtype)

    x_copy(0).wait()
    xt[0] = xraw[0].T.astype(BF16)

    @pl.when(has_left)
    def _():
        for g in range(GROUPS):
            back_copy(0, g).start()

    def transpose(w, row):
        for a in range(tiles):
            for b in range(a, tiles):
                ra, rb = pl.ds(a * TILE, TILE), pl.ds(b * TILE, TILE)
                upper = w[row, ra, rb]
                if a == b:
                    w[row, ra, rb] = upper.T
                else:
                    lower = w[row, rb, ra]
                    w[row, ra, rb] = lower.T
                    w[row, rb, ra] = upper.T

    def nds(n):
        return pl.ds(n * TILE, TILE)

    def product(x, lead, r, w, row):
        acc = [None] * tiles
        half = size // 2
        for h in range(2):
            ks = pl.ds(h * half, half)
            xv = x[(*lead, r, ks)]
            for n in range(tiles):
                part = jnp.dot(xv, w[row, ks, nds(n)], preferred_element_type=F32)
                acc[n] = part if acc[n] is None else acc[n] + part
        return acc

    def u_product(row, x, lead, dst, lead_dst):
        acc = product(x, lead, everything, wu, row)
        for n in range(tiles):
            dst[(*lead_dst, everything, nds(n))] = ft[row, :, nds(n)] - acc[n]

    def prep_fx(row, has_next):
        f_copy(row).wait()
        ft[row] = fraw[row].T
        if has_next:
            x_copy(row + 1).wait()
            xt[row + 1] = xraw[row + 1].T.astype(BF16)

    def finish_row(row, r, out_row=None):
        acc = product(tb, (), r, wd, row)
        for n in range(tiles):
            xt[row, r, nds(n)] = acc[n].astype(BF16)
            if out_row is not None:
                out[out_row, nds(n), r] = acc[n].T

    def store_t(r, base, lead, acc):
        for n in range(tiles):
            tb[r, nds(n)] = (base[(*lead, r, nds(n))] - acc[n]).astype(BF16)

    def issue_after_u(row):
        @pl.when(row + 1 < rows)
        def _():
            l_copy(row + 1).start()

    def issue_after_l(row):
        @pl.when(row + 1 < rows)
        def _():
            d_copy(row + 1).start()

    def issue_after_d(row):
        @pl.when(row + 2 < rows)
        def _():
            load_u(row + 2)

        @pl.when(row + 2 == rows)
        def _():
            l_copy(0).start()

    @pl.when(first)
    def _():
        prep_fx(0, True)
        u_copy(0).wait()
        d_copy(1).start()
        transpose(wu, 0)
        d_copy(0).wait()
        load_u(2)
        transpose(wd, 0)
        u_product(0, xt, (1,), tmp, ())
        for n in range(tiles):
            tb[:, nds(n)] = tmp[:, nds(n)].astype(BF16)

        def load_row(row, carry, has_next=True):
            prep_fx(row, has_next)
            u_copy(row).wait()
            issue_after_u(row)
            finish_row(row - 1, everything)
            transpose(wu, row)
            l_copy(row).wait()
            issue_after_l(row)
            if has_next:
                u_product(row, xt, (row + 1,), tmp, ())
            else:
                for g in range(GROUPS):
                    back_copy(0, g).wait_recv()
                u_product(row, rr, (0,), tmp, ())
            transpose(wl, row)
            d_copy(row).wait()
            issue_after_d(row)
            store_t(everything, tmp, (), product(xt, (row - 1,), everything, wl, row))
            transpose(wd, row)
            return carry

        lax.fori_loop(1, last_row, load_row, 0)
        load_row(last_row, 0, False)
        finish_row(last_row, everything)
        for g in range(GROUPS):
            fwd_copy(0, g).start()
        l_copy(0).wait()
        transpose(wl, 0)

        def u_pass(row, carry):
            u_product(row, xt, (row + 1,), st, (row,))
            return carry

        lax.fori_loop(0, last_row, u_pass, 0)

    @pl.when(jnp.logical_not(first))
    def _():
        prep_fx(0, True)
        u_copy(0).wait()
        d_copy(1).start()
        transpose(wu, 0)
        d_copy(0).wait()
        load_u(2)
        u_product(0, xt, (1,), st, (0,))
        transpose(wd, 0)

        def load_row(row, carry, has_next=True):
            prep_fx(row, has_next)
            u_copy(row).wait()
            issue_after_u(row)
            transpose(wu, row)
            l_copy(row).wait()
            issue_after_l(row)
            if has_next:
                u_product(row, xt, (row + 1,), st, (row,))
            transpose(wl, row)
            d_copy(row).wait()
            issue_after_d(row)
            transpose(wd, row)
            return carry

        lax.fori_loop(1, last_row, load_row, 0)
        load_row(last_row, 0, False)
        l_copy(0).wait()
        transpose(wl, 0)

    def sweep(k, last):
        def out_row(row):
            return row if last else None

        def recv_left(g):
            fwd_copy(k, g).wait_recv()

        def recv_right(g):
            back_copy(k, g).wait_recv()

        def send_left(g):
            if not last:
                back_copy(k + 1, g).start()

        @pl.when(pos == mid)
        def _():
            for g in range(GROUPS):
                recv_left(g)
                store_t(group(g), st, (0,), product(rl, (k,), group(g), wl, 0))
                back_copy(k, g).wait_send()
                finish_row(0, group(g), out_row(0))
                send_left(g)

        @pl.when(pos != mid)
        def _():
            @pl.when(has_left)
            def _():
                for g in range(GROUPS):
                    recv_left(g)
                    back_copy(k, g).wait_send()
            store_t(everything, st, (0,), product(rl, (k,), everything, wl, 0))
            finish_row(0, everything, out_row(0))

            @pl.when(has_left)
            def _():
                for g in range(GROUPS):
                    send_left(g)

        for row in range(1, last_row):
            store_t(everything, st, (row,), product(xt, (row - 1,), everything, wl, row))
            finish_row(row, everything, out_row(row))

        acc = product(xt, (last_row - 1,), everything, wl, last_row)
        for n in range(tiles):
            tmp[:, nds(n)] = ft[last_row, :, nds(n)] - acc[n]

        def wait_sent(g):
            if last:
                fwd_copy(k - 1, g).wait_send()
            else:
                @pl.when(k > 0)
                def _():
                    fwd_copy(k - 1, g).wait_send()

        @pl.when(pos == mid - 1)
        def _():
            for g in range(GROUPS):
                wait_sent(g)
            for g in range(GROUPS):
                recv_right(g)
                store_t(group(g), tmp, (), product(rr, (k,), group(g), wu, last_row))
                finish_row(last_row, group(g), out_row(last_row))
                fwd_copy(k, g).start()

        @pl.when(pos != mid - 1)
        def _():
            @pl.when(has_right)
            def _():
                for g in range(GROUPS):
                    wait_sent(g)
                    recv_right(g)
            store_t(everything, tmp, (), product(rr, (k,), everything, wu, last_row))
            finish_row(last_row, everything, out_row(last_row))

            @pl.when(has_right)
            def _():
                for g in range(GROUPS):
                    fwd_copy(k, g).start()

        if not last:
            for row in range(last_row):
                u_product(row, xt, (row + 1,), st, (row,))

    def mid_sweep(k, carry):
        sweep(k, False)
        return carry

    lax.fori_loop(first.astype(jnp.int32), SWEEPS - 1, mid_sweep, 0)
    sweep(SWEEPS - 1, True)

    @pl.when(has_right)
    def _():
        for g in range(GROUPS):
            fwd_copy(SWEEPS - 1, g).wait_send()


def solution(mesh):
    chain_len = mesh.shape["row"]
    mat_spec = P(("batch", "row"), None, None)
    vec_spec = P(("batch", "row"), None, "col")

    def device_fn(d_inv, l_blk, u_blk, rhs_blk, x_init):
        rows, size, cols = rhs_blk.shape
        any_spec = pl.BlockSpec(memory_space=pl.ANY)
        dma = pltpu.SemaphoreType.DMA
        return pl.pallas_call(
            lambda *refs: kernel(chain_len, *refs),
            out_shape=pltpu.VMEM(rhs_blk.shape, F32),
            in_specs=[any_spec] * 5,
            out_specs=pl.BlockSpec(memory_space=pltpu.VMEM),
            scratch_shapes=[
                pltpu.VMEM((rows, size, size), BF16),
                pltpu.VMEM((rows, size, size), BF16),
                pltpu.VMEM((rows, size, size), BF16),
                pltpu.VMEM((rows, size, cols), F32),
                pltpu.VMEM((rows, size, cols), F32),
                pltpu.VMEM((rows, cols, size), F32),
                pltpu.VMEM((rows, cols, size), F32),
                pltpu.VMEM((cols, size), F32),
                pltpu.VMEM((cols, size), BF16),
                pltpu.VMEM((rows, cols, size), BF16),
                pltpu.VMEM((SWEEPS, cols, size), BF16),
                pltpu.VMEM((SWEEPS, cols, size), BF16),
                dma((rows,)), dma((rows,)), dma((rows,)), dma((rows,)), dma((rows,)),
                dma((SWEEPS, GROUPS)), dma((SWEEPS, GROUPS)), dma((SWEEPS, GROUPS)), dma((SWEEPS, GROUPS)),
            ],
            compiler_params=pltpu.CompilerParams(
                collective_id=0, has_side_effects=True, vmem_limit_bytes=57 * 1024 * 1024),
        )(d_inv, l_blk, u_blk, rhs_blk, x_init)

    return jax.shard_map(device_fn, mesh=mesh, in_specs=(mat_spec, mat_spec, mat_spec, vec_spec, vec_spec),
                         out_specs=vec_spec, check_vma=False)
```

```python
import jax
import jax.numpy as jnp
from jax import lax
from jax.experimental import pallas as pl
from jax.experimental.pallas import tpu as pltpu
from jax.sharding import PartitionSpec as P

SWEEPS = 4
TILE = 256
GROUPS = (48, 48, 32)
HALVES = 2
MESH = pl.DeviceIdType.MESH
F32, BF16 = jnp.float32, jnp.bfloat16


def kernel(chain_len, d_hbm, l_hbm, u_hbm, f_hbm, x_hbm, out,
           wu, wl, wd, fraw, xraw, ft, st, tmp, tb, xt, rl, rr, eye,
           u_sem, l_sem, d_sem, f_sem, x_sem, fs_sem, fr_sem, bs_sem, br_sem):
    pos = lax.axis_index("row")
    rows, size, _ = d_hbm.shape
    cols = xt.shape[1]
    tiles = size // TILE
    half = size // HALVES
    first, has_left, has_right = pos == 0, pos > 0, pos < chain_len - 1
    mid = chain_len // 2
    last_row = rows - 1
    everything = pl.ds(0, cols)
    offsets = [sum(GROUPS[:g]) for g in range(len(GROUPS))]
    groups = range(len(GROUPS))
    halves = range(HALVES)

    def u_copy(row):
        return pltpu.make_async_copy(u_hbm.at[row], wu.at[row], u_sem.at[row])

    def l_copy(row):
        return pltpu.make_async_copy(l_hbm.at[row], wl.at[row], l_sem.at[row])

    def d_copy(row):
        return pltpu.make_async_copy(d_hbm.at[row], wd.at[row], d_sem.at[row])

    def f_copy(row):
        return pltpu.make_async_copy(f_hbm.at[row], fraw.at[row], f_sem.at[row])

    def x_copy(row):
        return pltpu.make_async_copy(x_hbm.at[row], xraw.at[row], x_sem.at[row])

    def group(g):
        return pl.ds(offsets[g], GROUPS[g])

    def hds(h):
        return pl.ds(h * half, half)

    def fwd_copy(k, g, h):
        return pltpu.make_async_remote_copy(
            src_ref=xt.at[last_row, group(g), hds(h)], dst_ref=rl.at[k, group(g), hds(h)],
            send_sem=fs_sem.at[k, g, h], recv_sem=fr_sem.at[k, g, h],
            device_id={"row": pos + 1}, device_id_type=MESH)

    def back_copy(k, g, h):
        return pltpu.make_async_remote_copy(
            src_ref=xt.at[0, group(g), hds(h)], dst_ref=rr.at[k, group(g), hds(h)],
            send_sem=bs_sem.at[k, g, h], recv_sem=br_sem.at[k, g, h],
            device_id={"row": pos - 1}, device_id_type=MESH)

    def load_u(row):
        f_copy(row).start()
        if isinstance(row, int):
            if row + 1 < rows:
                x_copy(row + 1).start()
        else:
            @pl.when(row + 1 < rows)
            def _():
                x_copy(row + 1).start()
        u_copy(row).start()

    x_copy(0).start()
    load_u(0)
    d_copy(0).start()
    load_u(1)
    l_copy(1).start()

    barrier = pltpu.get_barrier_semaphore()

    @pl.when(has_left)
    def _():
        pl.semaphore_signal(barrier, inc=1, device_id={"row": pos - 1}, device_id_type=MESH)

    @pl.when(has_right)
    def _():
        pl.semaphore_signal(barrier, inc=1, device_id={"row": pos + 1}, device_id_type=MESH)

    pl.semaphore_wait(barrier, has_left.astype(jnp.int32) + has_right.astype(jnp.int32))

    x_copy(0).wait()
    xt[0] = xraw[0].T.astype(BF16)

    @pl.when(has_left)
    def _():
        for g in groups:
            for h in halves:
                back_copy(0, g, h).start()

    def turned_by_matmul(v):
        return lax.dot_general(eye[...], v, (((1,), (1,)), ((), ())), preferred_element_type=F32).astype(BF16)

    def transpose_mixed(w, row, pairs):
        left = pairs
        for a in range(tiles):
            for b in range(a, tiles):
                ra, rb = pl.ds(a * TILE, TILE), pl.ds(b * TILE, TILE)
                upper = w[row, ra, rb]
                if a == b:
                    w[row, ra, rb] = turned_by_matmul(upper)
                else:
                    turn = turned_by_matmul if left > 0 else jnp.transpose
                    left -= 1
                    lower = w[row, rb, ra]
                    w[row, ra, rb] = turn(lower)
                    w[row, rb, ra] = turn(upper)

    def nds(n):
        return pl.ds(n * TILE, TILE)

    def partial(acc, h, x, lead, r, w, row, cols_of=None):
        xv = x[(*lead, r, hds(h))]
        for n in (range(tiles) if cols_of is None else cols_of):
            part = jnp.dot(xv, w[row, hds(h), nds(n)], preferred_element_type=F32)
            acc[n] = part if n not in acc else acc[n] + part

    def product(x, lead, r, w, row, cols_of=None):
        acc = {}
        for h in halves:
            partial(acc, h, x, lead, r, w, row, cols_of)
        return acc

    def store_sub(dst, lead_dst, r, base, lead, acc, dtype=F32):
        for n in acc:
            dst[(*lead_dst, r, nds(n))] = (base[(*lead, r, nds(n))] - acc[n]).astype(dtype)

    def store_t(r, base, lead, acc):
        store_sub(tb, (), r, base, lead, acc, BF16)

    def u_product(row, cols_of=None):
        store_sub(st, (row,), everything, ft, (row,), product(xt, (row + 1,), everything, wu, row, cols_of))

    def finish_part(row, r, acc, last):
        for n in acc:
            xt[row, r, nds(n)] = acc[n].astype(BF16)
            if last and r is everything:
                out[row, nds(n), :] = acc[n].T
            elif last:
                st[row, r, nds(n)] = acc[n]

    def finish_row(row, r, last):
        finish_part(row, r, product(tb, (), r, wd, row), last)

    def finish_and_send(row, r, last, send):
        acc = product(tb, (), r, wd, row, range(tiles // 2))
        acc2 = product(tb, (), r, wd, row, range(tiles // 2, tiles))
        finish_part(row, r, acc, last)
        send(0)
        finish_part(row, r, acc2, last)
        send(1)

    def issue_after_u(row):
        @pl.when(row + 1 < rows)
        def _():
            l_copy(row + 1).start()

    def issue_after_l(row):
        @pl.when(row + 1 < rows)
        def _():
            d_copy(row + 1).start()

    def issue_after_d(row):
        @pl.when(row + 2 < rows)
        def _():
            load_u(row + 2)

        @pl.when(row + 2 == rows)
        def _():
            l_copy(0).start()

    spare = rows + 1

    def wait_fx(row):
        @pl.when(row < rows)
        def _():
            f_copy(row).wait()

        @pl.when(row + 1 < rows)
        def _():
            x_copy(row + 1).wait()

    def turn_fx(row):
        src = jnp.minimum(row, last_row)
        ft[src] = fraw[src].T
        x_src = jnp.minimum(row + 1, last_row)
        xt[jnp.where(row + 1 < rows, row + 1, spare)] = xraw[x_src].T.astype(BF16)

    eye[...] = (lax.broadcasted_iota(jnp.int32, eye.shape, 0)
                == lax.broadcasted_iota(jnp.int32, eye.shape, 1)).astype(F32).astype(BF16)
    def take_right(row):
        @pl.when(has_right & (row == last_row))
        def _():
            for g in groups:
                for h in halves:
                    back_copy(0, g, h).wait_recv()
            xt[rows] = rr[0]

        @pl.when(jnp.logical_not(has_right) & (row == last_row))
        def _():
            xt[rows] = jnp.zeros(xt.shape[1:], xt.dtype)

    f_copy(0).wait()
    ft[0] = fraw[0].T
    x_copy(1).wait()
    xt[1] = xraw[1].T.astype(BF16)

    @pl.when(first)
    def _():
        u_copy(0).wait()
        d_copy(1).start()
        transpose_mixed(wu, 0, 2)
        d_copy(0).wait()
        load_u(2)
        wait_fx(1)
        acc = product(xt, (1,), everything, wu, 0)
        for n in range(tiles):
            tb[:, nds(n)] = (ft[0, :, nds(n)] - acc[n]).astype(BF16)
        transpose_mixed(wd, 0, 1)
        turn_fx(1)

        def load_row(row, carry):
            take_right(row)
            u_copy(row).wait()
            issue_after_u(row)
            finish_row(row - 1, everything, False)
            transpose_mixed(wu, row, 1)
            l_copy(row).wait()
            issue_after_l(row)
            store_sub(tmp, (), everything, ft, (row,), product(xt, (row + 1,), everything, wu, row))
            transpose_mixed(wl, row, 1)
            d_copy(row).wait()
            issue_after_d(row)
            wait_fx(row + 1)
            store_t(everything, tmp, (), product(xt, (row - 1,), everything, wl, row))
            transpose_mixed(wd, row, 2)
            turn_fx(row + 1)
            return carry

        lax.fori_loop(1, rows, load_row, 0)
        finish_row(last_row, everything, False)
        for g in groups:
            for h in halves:
                fwd_copy(0, g, h).start()
        l_copy(0).wait()
        transpose_mixed(wl, 0, 2)
        for row in range(last_row):
            u_product(row)

    @pl.when(jnp.logical_not(first))
    def _():
        u_copy(0).wait()
        d_copy(1).start()
        transpose_mixed(wu, 0, 2)
        d_copy(0).wait()
        load_u(2)
        wait_fx(1)
        u_product(0)
        transpose_mixed(wd, 0, 1)
        turn_fx(1)

        def load_row(row, carry):
            take_right(row)
            u_copy(row).wait()
            issue_after_u(row)
            transpose_mixed(wu, row, 1)
            l_copy(row).wait()
            issue_after_l(row)
            u_product(row)
            transpose_mixed(wl, row, 1)
            d_copy(row).wait()
            issue_after_d(row)
            wait_fx(row + 1)
            transpose_mixed(wd, row, 2)
            turn_fx(row + 1)
            return carry

        lax.fori_loop(1, rows, load_row, 0)
        l_copy(0).wait()
        transpose_mixed(wl, 0, 2)

    by_group = [(group(g), (g,)) for g in groups]
    at_once = [(everything, tuple(groups))]

    def first_row(k, parts, last):
        for r, members in parts:
            acc = {}
            for h in halves:
                for g in members:
                    fwd_copy(k, g, h).wait_recv()
                partial(acc, h, rl, (k,), r, wl, 0)
            store_t(r, st, (0,), acc)
            for g in members:
                for h in halves:
                    back_copy(k, g, h).wait_send()

            def send(h):
                if not last:
                    for g in members:
                        back_copy(k + 1, g, h).start()

            finish_and_send(0, r, last, send)

    def last_row_plain(k, last, send):
        store_t(everything, st, (last_row,), product(xt, (last_row - 1,), everything, wl, last_row))
        finish_row(last_row, everything, last)
        if send:
            for g in groups:
                for h in halves:
                    fwd_copy(k, g, h).start()

    def take_last_u(k):
        for g in groups:
            for h in halves:
                back_copy(k, g, h).wait_recv()
        store_sub(st, (last_row,), everything, ft, (last_row,),
                  product(rr, (k,), everything, wu, last_row))

    def turn_out(row):
        for n in range(tiles):
            out[row, nds(n), :] = st[row, :, nds(n)].T

    def sweep(k, last):
        @pl.when(first)
        def _():
            for n in range(tiles):
                tb[:, nds(n)] = st[0, :, nds(n)].astype(BF16)
            finish_row(0, everything, last)

        @pl.when(pos == mid)
        def _():
            first_row(k, by_group, last)
            if last:
                turn_out(0)

        @pl.when(has_left & (pos != mid))
        def _():
            first_row(k, at_once, last)

        for row in range(1, last_row):
            store_t(everything, st, (row,), product(xt, (row - 1,), everything, wl, row))
            if row > 1 and not last:
                u_product(row - 2, range(tiles // 2))
            finish_row(row, everything, last)
            if row > 1 and not last:
                u_product(row - 2, range(tiles // 2, tiles))

        @pl.when(has_right & (k > 0))
        def _():
            for g in groups:
                for h in halves:
                    fwd_copy(k - 1, g, h).wait_send()

        @pl.when((pos == mid - 1) & (k > 0))
        def _():
            store_sub(tmp, (), everything, ft, (last_row,),
                      product(xt, (last_row - 1,), everything, wl, last_row))
            for r, members in by_group:
                acc = {}
                for h in halves:
                    for g in members:
                        back_copy(k, g, h).wait_recv()
                    partial(acc, h, rr, (k,), r, wu, last_row)
                store_t(r, tmp, (), acc)

                def send(h):
                    for g in members:
                        fwd_copy(k, g, h).start()

                finish_and_send(last_row, r, last, send)
            if last:
                turn_out(last_row)

        @pl.when(has_right & (pos != mid - 1) & (k > 0))
        def _():
            take_last_u(k)

        @pl.when(has_right & ((pos != mid - 1) | (k == 0)))
        def _():
            last_row_plain(k, last, True)

        @pl.when(jnp.logical_not(has_right))
        def _():
            last_row_plain(k, last, False)

        if not last:
            for row in range(last_row - 2, last_row):
                u_product(row)

    def mid_sweep(k, carry):
        sweep(k, False)
        return carry

    lax.fori_loop(first.astype(jnp.int32), SWEEPS - 1, mid_sweep, 0)
    sweep(SWEEPS - 1, True)

    @pl.when(has_right)
    def _():
        for g in groups:
            for h in halves:
                fwd_copy(SWEEPS - 1, g, h).wait_send()


def solution(mesh):
    chain_len = mesh.shape["row"]
    mat_spec = P(("batch", "row"), None, None)
    vec_spec = P(("batch", "row"), None, "col")

    def device_fn(d_inv, l_blk, u_blk, rhs_blk, x_init):
        rows, size, cols = rhs_blk.shape
        any_spec = pl.BlockSpec(memory_space=pl.ANY)
        dma = pltpu.SemaphoreType.DMA
        return pl.pallas_call(
            lambda *refs: kernel(chain_len, *refs),
            out_shape=pltpu.VMEM(rhs_blk.shape, F32),
            in_specs=[any_spec] * 5,
            out_specs=pl.BlockSpec(memory_space=pltpu.VMEM),
            scratch_shapes=[
                pltpu.VMEM((rows, size, size), BF16),
                pltpu.VMEM((rows, size, size), BF16),
                pltpu.VMEM((rows, size, size), BF16),
                pltpu.VMEM((rows, size, cols), F32),
                pltpu.VMEM((rows, size, cols), F32),
                pltpu.VMEM((rows, cols, size), F32),
                pltpu.VMEM((rows, cols, size), F32),
                pltpu.VMEM((cols, size), F32),
                pltpu.VMEM((cols, size), BF16),
                pltpu.VMEM((rows + 2, cols, size), BF16),
                pltpu.VMEM((SWEEPS, cols, size), BF16),
                pltpu.VMEM((SWEEPS, cols, size), BF16),
                pltpu.VMEM((TILE, TILE), BF16),
                dma((rows,)), dma((rows,)), dma((rows,)), dma((rows,)), dma((rows,)),
                *[dma((SWEEPS, len(GROUPS), HALVES))] * 4,
            ],
            compiler_params=pltpu.CompilerParams(
                collective_id=0, has_side_effects=True,
                vmem_limit_bytes=57 * 1024 * 1024),
        )(d_inv, l_blk, u_blk, rhs_blk, x_init)

    return jax.shard_map(device_fn, mesh=mesh, in_specs=(mat_spec, mat_spec, mat_spec, vec_spec, vec_spec),
                         out_specs=vec_spec, check_vma=False)
```

```python
import jax
import jax.numpy as jnp
from jax import lax
from jax.experimental import pallas as pl
from jax.experimental.pallas import tpu as pltpu
from jax.sharding import PartitionSpec as P

SWEEPS = 4
TILE = 256
GROUPS = (48, 48, 32)
HALVES = 1
MESH = pl.DeviceIdType.MESH
F32, BF16 = jnp.float32, jnp.bfloat16


def kernel(chain_len, d_hbm, l_hbm, u_hbm, f_hbm, x_hbm, out,
           wu, wl, wd, fraw, xraw, ft, st, tmp, tb, xt, rl, rr, eye,
           u_sem, l_sem, d_sem, f_sem, x_sem, fs_sem, fr_sem, bs_sem, br_sem):
    pos = lax.axis_index("row")
    rows, size, _ = d_hbm.shape
    cols = xt.shape[1]
    tiles = size // TILE
    half = size // HALVES
    first, has_left, has_right = pos == 0, pos > 0, pos < chain_len - 1
    mid = chain_len // 2
    last_row = rows - 1
    everything = pl.ds(0, cols)
    offsets = [sum(GROUPS[:g]) for g in range(len(GROUPS))]
    groups = range(len(GROUPS))
    halves = range(HALVES)

    def u_copy(row):
        return pltpu.make_async_copy(u_hbm.at[row], wu.at[row], u_sem.at[row])

    def l_copy(row):
        return pltpu.make_async_copy(l_hbm.at[row], wl.at[row], l_sem.at[row])

    def d_copy(row):
        return pltpu.make_async_copy(d_hbm.at[row], wd.at[row], d_sem.at[row])

    def f_copy(row):
        return pltpu.make_async_copy(f_hbm.at[row], fraw.at[row], f_sem.at[row])

    def x_copy(row):
        return pltpu.make_async_copy(x_hbm.at[row], xraw.at[row], x_sem.at[row])

    def group(g):
        return pl.ds(offsets[g], GROUPS[g])

    def hds(h):
        return pl.ds(h * half, half)

    def fwd_copy(k, g, h):
        return pltpu.make_async_remote_copy(
            src_ref=xt.at[last_row, group(g), hds(h)], dst_ref=rl.at[k, group(g), hds(h)],
            send_sem=fs_sem.at[k, g, h], recv_sem=fr_sem.at[k, g, h],
            device_id={"row": pos + 1}, device_id_type=MESH)

    def back_copy(k, g, h):
        return pltpu.make_async_remote_copy(
            src_ref=xt.at[0, group(g), hds(h)], dst_ref=rr.at[k, group(g), hds(h)],
            send_sem=bs_sem.at[k, g, h], recv_sem=br_sem.at[k, g, h],
            device_id={"row": pos - 1}, device_id_type=MESH)

    def load_u(row):
        f_copy(row).start()
        if isinstance(row, int):
            if row + 1 < rows:
                x_copy(row + 1).start()
        else:
            @pl.when(row + 1 < rows)
            def _():
                x_copy(row + 1).start()
        u_copy(row).start()

    x_copy(0).start()
    load_u(0)
    d_copy(0).start()
    load_u(1)
    l_copy(1).start()

    barrier = pltpu.get_barrier_semaphore()

    @pl.when(has_left)
    def _():
        pl.semaphore_signal(barrier, inc=1, device_id={"row": pos - 1}, device_id_type=MESH)

    @pl.when(has_right)
    def _():
        pl.semaphore_signal(barrier, inc=1, device_id={"row": pos + 1}, device_id_type=MESH)

    pl.semaphore_wait(barrier, has_left.astype(jnp.int32) + has_right.astype(jnp.int32))

    x_copy(0).wait()
    xt[0] = xraw[0].T.astype(BF16)

    @pl.when(has_left)
    def _():
        for g in groups:
            for h in halves:
                back_copy(0, g, h).start()

    def turned_by_matmul(v):
        return lax.dot_general(eye[...], v, (((1,), (1,)), ((), ())), preferred_element_type=F32).astype(BF16)

    def transpose_mixed(w, row, pairs):
        left = pairs
        for a in range(tiles):
            for b in range(a, tiles):
                ra, rb = pl.ds(a * TILE, TILE), pl.ds(b * TILE, TILE)
                upper = w[row, ra, rb]
                if a == b:
                    w[row, ra, rb] = turned_by_matmul(upper)
                else:
                    turn = turned_by_matmul if left > 0 else jnp.transpose
                    left -= 1
                    lower = w[row, rb, ra]
                    w[row, ra, rb] = turn(lower)
                    w[row, rb, ra] = turn(upper)

    def nds(n):
        return pl.ds(n * TILE, TILE)

    def product(x, lead, r, w, row, cols_of=None):
        xv = x[(*lead, r)]
        return {n: jnp.dot(xv, w[row, :, nds(n)], preferred_element_type=F32)
                for n in (range(tiles) if cols_of is None else cols_of)}

    def store_sub(dst, lead_dst, r, base, lead, acc, dtype=F32):
        for n in acc:
            dst[(*lead_dst, r, nds(n))] = (base[(*lead, r, nds(n))] - acc[n]).astype(dtype)

    def store_t(r, base, lead, acc):
        store_sub(tb, (), r, base, lead, acc, BF16)

    def u_product(row, cols_of=None):
        store_sub(st, (row,), everything, ft, (row,), product(xt, (row + 1,), everything, wu, row, cols_of))

    def finish_part(row, r, acc, last):
        for n in acc:
            xt[row, r, nds(n)] = acc[n].astype(BF16)
            if last and r is everything:
                out[row, nds(n), :] = acc[n].T
            elif last:
                st[row, r, nds(n)] = acc[n]

    def finish_row(row, r, last):
        finish_part(row, r, product(tb, (), r, wd, row), last)

    def finish_and_send(row, r, last, send):
        finish_row(row, r, last)
        for h in halves:
            send(h)

    def issue_after_u(row):
        @pl.when(row + 1 < rows)
        def _():
            l_copy(row + 1).start()

    def issue_after_l(row):
        @pl.when(row + 1 < rows)
        def _():
            d_copy(row + 1).start()

    def issue_after_d(row):
        @pl.when(row + 2 < rows)
        def _():
            load_u(row + 2)

        @pl.when(row + 2 == rows)
        def _():
            l_copy(0).start()

    spare = rows + 1

    def wait_fx(row):
        @pl.when(row < rows)
        def _():
            f_copy(row).wait()

        @pl.when(row + 1 < rows)
        def _():
            x_copy(row + 1).wait()

    def turn_fx(row):
        src = jnp.minimum(row, last_row)
        ft[src] = fraw[src].T
        x_src = jnp.minimum(row + 1, last_row)
        xt[jnp.where(row + 1 < rows, row + 1, spare)] = xraw[x_src].T.astype(BF16)

    eye[...] = (lax.broadcasted_iota(jnp.int32, eye.shape, 0)
                == lax.broadcasted_iota(jnp.int32, eye.shape, 1)).astype(F32).astype(BF16)
    def take_right(row):
        @pl.when(has_right & (row == last_row))
        def _():
            for g in groups:
                for h in halves:
                    back_copy(0, g, h).wait_recv()
            xt[rows] = rr[0]

        @pl.when(jnp.logical_not(has_right) & (row == last_row))
        def _():
            xt[rows] = jnp.zeros(xt.shape[1:], xt.dtype)

    f_copy(0).wait()
    ft[0] = fraw[0].T
    x_copy(1).wait()
    xt[1] = xraw[1].T.astype(BF16)

    @pl.when(first)
    def _():
        u_copy(0).wait()
        d_copy(1).start()
        transpose_mixed(wu, 0, 2)
        d_copy(0).wait()
        load_u(2)
        wait_fx(1)
        acc = product(xt, (1,), everything, wu, 0)
        for n in range(tiles):
            tb[:, nds(n)] = (ft[0, :, nds(n)] - acc[n]).astype(BF16)
        transpose_mixed(wd, 0, 1)
        turn_fx(1)

        def load_row(row, carry):
            take_right(row)
            u_copy(row).wait()
            issue_after_u(row)
            finish_row(row - 1, everything, False)
            transpose_mixed(wu, row, 1)
            l_copy(row).wait()
            issue_after_l(row)
            store_sub(tmp, (), everything, ft, (row,), product(xt, (row + 1,), everything, wu, row))
            transpose_mixed(wl, row, 1)
            d_copy(row).wait()
            issue_after_d(row)
            wait_fx(row + 1)
            store_t(everything, tmp, (), product(xt, (row - 1,), everything, wl, row))
            transpose_mixed(wd, row, 2)
            turn_fx(row + 1)
            return carry

        lax.fori_loop(1, rows, load_row, 0)
        finish_row(last_row, everything, False)
        for g in groups:
            for h in halves:
                fwd_copy(0, g, h).start()
        l_copy(0).wait()
        transpose_mixed(wl, 0, 2)
        for row in range(last_row):
            u_product(row)

    @pl.when(jnp.logical_not(first))
    def _():
        u_copy(0).wait()
        d_copy(1).start()
        transpose_mixed(wu, 0, 2)
        d_copy(0).wait()
        load_u(2)
        wait_fx(1)
        u_product(0)
        transpose_mixed(wd, 0, 1)
        turn_fx(1)

        def load_row(row, carry):
            take_right(row)
            u_copy(row).wait()
            issue_after_u(row)
            transpose_mixed(wu, row, 1)
            l_copy(row).wait()
            issue_after_l(row)
            u_product(row)
            transpose_mixed(wl, row, 1)
            d_copy(row).wait()
            issue_after_d(row)
            wait_fx(row + 1)
            transpose_mixed(wd, row, 2)
            turn_fx(row + 1)
            return carry

        lax.fori_loop(1, rows, load_row, 0)
        l_copy(0).wait()
        transpose_mixed(wl, 0, 2)

    by_group = [(group(g), (g,)) for g in groups]
    at_once = [(everything, tuple(groups))]

    def first_row(k, parts, last):
        for r, members in parts:
            for h in halves:
                for g in members:
                    fwd_copy(k, g, h).wait_recv()
            store_t(r, st, (0,), product(rl, (k,), r, wl, 0))
            for g in members:
                for h in halves:
                    back_copy(k, g, h).wait_send()

            def send(h):
                if not last:
                    for g in members:
                        back_copy(k + 1, g, h).start()

            finish_and_send(0, r, last, send)

    def last_row_plain(k, last, send):
        store_t(everything, st, (last_row,), product(xt, (last_row - 1,), everything, wl, last_row))
        finish_row(last_row, everything, last)
        if send:
            for g in groups:
                for h in halves:
                    fwd_copy(k, g, h).start()

    def take_last_u(k):
        for g in groups:
            for h in halves:
                back_copy(k, g, h).wait_recv()
        store_sub(st, (last_row,), everything, ft, (last_row,),
                  product(rr, (k,), everything, wu, last_row))

    def turn_out(row):
        for n in range(tiles):
            out[row, nds(n), :] = st[row, :, nds(n)].T

    def sweep(k, last):
        @pl.when(first)
        def _():
            for n in range(tiles):
                tb[:, nds(n)] = st[0, :, nds(n)].astype(BF16)
            finish_row(0, everything, last)

        @pl.when(pos == mid)
        def _():
            first_row(k, by_group, last)
            if last:
                turn_out(0)

        @pl.when(has_left & (pos != mid))
        def _():
            first_row(k, at_once, last)

        for row in range(1, last_row):
            store_t(everything, st, (row,), product(xt, (row - 1,), everything, wl, row))
            if row > 1 and not last:
                u_product(row - 2, range(tiles // 2))
            finish_row(row, everything, last)
            if row > 1 and not last:
                u_product(row - 2, range(tiles // 2, tiles))

        @pl.when(has_right & (k > 0))
        def _():
            for g in groups:
                for h in halves:
                    fwd_copy(k - 1, g, h).wait_send()

        @pl.when((pos == mid - 1) & (k > 0))
        def _():
            store_sub(tmp, (), everything, ft, (last_row,),
                      product(xt, (last_row - 1,), everything, wl, last_row))
            for r, members in by_group:
                for h in halves:
                    for g in members:
                        back_copy(k, g, h).wait_recv()
                store_t(r, tmp, (), product(rr, (k,), r, wu, last_row))

                def send(h):
                    for g in members:
                        fwd_copy(k, g, h).start()

                finish_and_send(last_row, r, last, send)
            if last:
                turn_out(last_row)

        @pl.when(has_right & (pos != mid - 1) & (k > 0))
        def _():
            take_last_u(k)

        @pl.when(has_right & ((pos != mid - 1) | (k == 0)))
        def _():
            last_row_plain(k, last, True)

        @pl.when(jnp.logical_not(has_right))
        def _():
            last_row_plain(k, last, False)

        if not last:
            for row in range(last_row - 2, last_row):
                u_product(row)

    def mid_sweep(k, carry):
        sweep(k, False)
        return carry

    lax.fori_loop(first.astype(jnp.int32), SWEEPS - 1, mid_sweep, 0)
    sweep(SWEEPS - 1, True)

    @pl.when(has_right)
    def _():
        for g in groups:
            for h in halves:
                fwd_copy(SWEEPS - 1, g, h).wait_send()


def solution(mesh):
    chain_len = mesh.shape["row"]
    mat_spec = P(("batch", "row"), None, None)
    vec_spec = P(("batch", "row"), None, "col")

    def device_fn(d_inv, l_blk, u_blk, rhs_blk, x_init):
        rows, size, cols = rhs_blk.shape
        any_spec = pl.BlockSpec(memory_space=pl.ANY)
        dma = pltpu.SemaphoreType.DMA
        return pl.pallas_call(
            lambda *refs: kernel(chain_len, *refs),
            out_shape=pltpu.VMEM(rhs_blk.shape, F32),
            in_specs=[any_spec] * 5,
            out_specs=pl.BlockSpec(memory_space=pltpu.VMEM),
            scratch_shapes=[
                pltpu.VMEM((rows, size, size), BF16),
                pltpu.VMEM((rows, size, size), BF16),
                pltpu.VMEM((rows, size, size), BF16),
                pltpu.VMEM((rows, size, cols), F32),
                pltpu.VMEM((rows, size, cols), F32),
                pltpu.VMEM((rows, cols, size), F32),
                pltpu.VMEM((rows, cols, size), F32),
                pltpu.VMEM((cols, size), F32),
                pltpu.VMEM((cols, size), BF16),
                pltpu.VMEM((rows + 2, cols, size), BF16),
                pltpu.VMEM((SWEEPS, cols, size), BF16),
                pltpu.VMEM((SWEEPS, cols, size), BF16),
                pltpu.VMEM((TILE, TILE), BF16),
                dma((rows,)), dma((rows,)), dma((rows,)), dma((rows,)), dma((rows,)),
                *[dma((SWEEPS, len(GROUPS), HALVES))] * 4,
            ],
            compiler_params=pltpu.CompilerParams(
                collective_id=0, has_side_effects=True,
                vmem_limit_bytes=57 * 1024 * 1024),
        )(d_inv, l_blk, u_blk, rhs_blk, x_init)

    return jax.shard_map(device_fn, mesh=mesh, in_specs=(mat_spec, mat_spec, mat_spec, vec_spec, vec_spec),
                         out_specs=vec_spec, check_vma=False)
```

```python
import jax
import jax.numpy as jnp
from jax import lax
from jax.experimental import pallas as pl
from jax.experimental.pallas import tpu as pltpu
from jax.sharding import PartitionSpec as P

SWEEPS = 4
TILE = 256
GROUPS = (48, 48, 32)
HALVES = 1
MESH = pl.DeviceIdType.MESH
F32, BF16 = jnp.float32, jnp.bfloat16


def kernel(chain_len, d_hbm, l_hbm, u_hbm, f_hbm, x_hbm, out,
           wu, wl, wd, fraw, xraw, ft, st, tmp, tb, xt, rl, rr, eye,
           u_sem, l_sem, d_sem, f_sem, x_sem, fs_sem, fr_sem, bs_sem, br_sem):
    pos = lax.axis_index("row")
    rows, size, _ = d_hbm.shape
    cols = xt.shape[1]
    tiles = size // TILE
    half = size // HALVES
    first, has_left, has_right = pos == 0, pos > 0, pos < chain_len - 1
    mid = chain_len // 2
    last_row = rows - 1
    everything = pl.ds(0, cols)
    offsets = [sum(GROUPS[:g]) for g in range(len(GROUPS))]
    groups = range(len(GROUPS))
    halves = range(HALVES)

    def u_copy(row):
        return pltpu.make_async_copy(u_hbm.at[row], wu.at[row], u_sem.at[row])

    def l_copy(row):
        return pltpu.make_async_copy(l_hbm.at[row], wl.at[row], l_sem.at[row])

    def d_copy(row):
        return pltpu.make_async_copy(d_hbm.at[row], wd.at[row], d_sem.at[row])

    def f_copy(row):
        return pltpu.make_async_copy(f_hbm.at[row], fraw.at[row], f_sem.at[row])

    def x_copy(row):
        return pltpu.make_async_copy(x_hbm.at[row], xraw.at[row], x_sem.at[row])

    def group(g):
        return pl.ds(offsets[g], GROUPS[g])

    def hds(h):
        return pl.ds(h * half, half)

    def fwd_copy(k, g, h):
        return pltpu.make_async_remote_copy(
            src_ref=xt.at[last_row, group(g), hds(h)], dst_ref=rl.at[k, group(g), hds(h)],
            send_sem=fs_sem.at[k, g, h], recv_sem=fr_sem.at[k, g, h],
            device_id={"row": pos + 1}, device_id_type=MESH)

    def back_copy(k, g, h):
        return pltpu.make_async_remote_copy(
            src_ref=xt.at[0, group(g), hds(h)], dst_ref=rr.at[k, group(g), hds(h)],
            send_sem=bs_sem.at[k, g, h], recv_sem=br_sem.at[k, g, h],
            device_id={"row": pos - 1}, device_id_type=MESH)

    def load_u(row):
        f_copy(row).start()
        if isinstance(row, int):
            if row + 1 < rows:
                x_copy(row + 1).start()
        else:
            @pl.when(row + 1 < rows)
            def _():
                x_copy(row + 1).start()
        u_copy(row).start()

    @pl.when(has_left)
    def _():
        x_copy(0).start()

    load_u(0)
    d_copy(0).start()
    load_u(1)
    l_copy(1).start()

    barrier = pltpu.get_barrier_semaphore()

    @pl.when(has_left)
    def _():
        pl.semaphore_signal(barrier, inc=1, device_id={"row": pos - 1}, device_id_type=MESH)

    @pl.when(has_right)
    def _():
        pl.semaphore_signal(barrier, inc=1, device_id={"row": pos + 1}, device_id_type=MESH)

    pl.semaphore_wait(barrier, has_left.astype(jnp.int32) + has_right.astype(jnp.int32))

    @pl.when(has_left)
    def _():
        x_copy(0).wait()
        xt[0] = xraw[0].T.astype(BF16)
        for g in groups:
            for h in halves:
                back_copy(0, g, h).start()

    def turned_by_matmul(v):
        return lax.dot_general(eye[...], v, (((1,), (1,)), ((), ())), preferred_element_type=F32).astype(BF16)

    def transpose_mixed(w, row, pairs):
        left = pairs
        for a in range(tiles):
            for b in range(a, tiles):
                ra, rb = pl.ds(a * TILE, TILE), pl.ds(b * TILE, TILE)
                upper = w[row, ra, rb]
                if a == b:
                    w[row, ra, rb] = turned_by_matmul(upper)
                else:
                    turn = turned_by_matmul if left > 0 else jnp.transpose
                    left -= 1
                    lower = w[row, rb, ra]
                    w[row, ra, rb] = turn(lower)
                    w[row, rb, ra] = turn(upper)

    def nds(n):
        return pl.ds(n * TILE, TILE)

    def product(x, lead, r, w, row, cols_of=None):
        xv = x[(*lead, r)]
        return {n: jnp.dot(xv, w[row, :, nds(n)], preferred_element_type=F32)
                for n in (range(tiles) if cols_of is None else cols_of)}

    def store_sub(dst, lead_dst, r, base, lead, acc, dtype=F32):
        for n in acc:
            dst[(*lead_dst, r, nds(n))] = (base[(*lead, r, nds(n))] - acc[n]).astype(dtype)

    def store_t(r, base, lead, acc):
        store_sub(tb, (), r, base, lead, acc, BF16)

    def u_product(row, cols_of=None):
        store_sub(st, (row,), everything, ft, (row,), product(xt, (row + 1,), everything, wu, row, cols_of))

    def finish_part(row, r, acc, last):
        for n in acc:
            xt[row, r, nds(n)] = acc[n].astype(BF16)
            if last and r is everything:
                out[row, nds(n), :] = acc[n].T
            elif last:
                st[row, r, nds(n)] = acc[n]

    def finish_row(row, r, last):
        finish_part(row, r, product(tb, (), r, wd, row), last)

    def finish_and_send(row, r, last, send):
        finish_row(row, r, last)
        for h in halves:
            send(h)

    def issue_after_u(row):
        @pl.when(row + 1 < rows)
        def _():
            l_copy(row + 1).start()

    def issue_after_l(row):
        @pl.when(row + 1 < rows)
        def _():
            d_copy(row + 1).start()

    def issue_after_d(row):
        @pl.when(row + 2 < rows)
        def _():
            load_u(row + 2)

        @pl.when(row + 2 == rows)
        def _():
            l_copy(0).start()

    spare = rows + 1

    def wait_fx(row):
        @pl.when(row < rows)
        def _():
            f_copy(row).wait()

        @pl.when(row + 1 < rows)
        def _():
            x_copy(row + 1).wait()

    def turn_fx(row):
        src = jnp.minimum(row, last_row)
        ft[src] = fraw[src].T
        x_src = jnp.minimum(row + 1, last_row)
        xt[jnp.where(row + 1 < rows, row + 1, spare)] = xraw[x_src].T.astype(BF16)

    eye[...] = (lax.broadcasted_iota(jnp.int32, eye.shape, 0)
                == lax.broadcasted_iota(jnp.int32, eye.shape, 1)).astype(F32).astype(BF16)
    def take_right(row):
        @pl.when(has_right & (row == last_row))
        def _():
            for g in groups:
                for h in halves:
                    back_copy(0, g, h).wait_recv()
            xt[rows] = rr[0]

        @pl.when(jnp.logical_not(has_right) & (row == last_row))
        def _():
            xt[rows] = jnp.zeros(xt.shape[1:], xt.dtype)

    f_copy(0).wait()
    ft[0] = fraw[0].T
    x_copy(1).wait()
    xt[1] = xraw[1].T.astype(BF16)

    @pl.when(first)
    def _():
        u_copy(0).wait()
        d_copy(1).start()
        transpose_mixed(wu, 0, 2)
        d_copy(0).wait()
        load_u(2)
        wait_fx(1)
        acc = product(xt, (1,), everything, wu, 0)
        for n in range(tiles):
            tb[:, nds(n)] = (ft[0, :, nds(n)] - acc[n]).astype(BF16)
        transpose_mixed(wd, 0, 1)
        turn_fx(1)

        def load_row(row, carry):
            take_right(row)
            u_copy(row).wait()
            issue_after_u(row)
            finish_row(row - 1, everything, False)
            transpose_mixed(wu, row, 1)
            l_copy(row).wait()
            issue_after_l(row)
            store_sub(tmp, (), everything, ft, (row,), product(xt, (row + 1,), everything, wu, row))
            transpose_mixed(wl, row, 1)
            d_copy(row).wait()
            issue_after_d(row)
            wait_fx(row + 1)
            store_t(everything, tmp, (), product(xt, (row - 1,), everything, wl, row))
            transpose_mixed(wd, row, 2)
            turn_fx(row + 1)
            return carry

        lax.fori_loop(1, rows, load_row, 0)
        finish_row(last_row, everything, False)
        for g in groups:
            for h in halves:
                fwd_copy(0, g, h).start()
        l_copy(0).wait()
        transpose_mixed(wl, 0, 2)
        for row in range(last_row):
            u_product(row)

    @pl.when(jnp.logical_not(first))
    def _():
        u_copy(0).wait()
        d_copy(1).start()
        transpose_mixed(wu, 0, 2)
        d_copy(0).wait()
        load_u(2)
        wait_fx(1)
        u_product(0)
        transpose_mixed(wd, 0, 1)
        turn_fx(1)

        def load_row(row, carry):
            take_right(row)
            u_copy(row).wait()
            issue_after_u(row)
            transpose_mixed(wu, row, 1)
            l_copy(row).wait()
            issue_after_l(row)
            u_product(row)
            transpose_mixed(wl, row, 1)
            d_copy(row).wait()
            issue_after_d(row)
            wait_fx(row + 1)
            transpose_mixed(wd, row, 2)
            turn_fx(row + 1)
            return carry

        lax.fori_loop(1, rows, load_row, 0)
        l_copy(0).wait()
        transpose_mixed(wl, 0, 2)

    by_group = [(group(g), (g,)) for g in groups]
    at_once = [(everything, tuple(groups))]

    def first_row(k, parts, last):
        for r, members in parts:
            for h in halves:
                for g in members:
                    fwd_copy(k, g, h).wait_recv()
            store_t(r, st, (0,), product(rl, (k,), r, wl, 0))
            for g in members:
                for h in halves:
                    back_copy(k, g, h).wait_send()

            def send(h):
                if not last:
                    for g in members:
                        back_copy(k + 1, g, h).start()

            finish_and_send(0, r, last, send)

    def last_row_plain(k, last, send):
        store_t(everything, st, (last_row,), product(xt, (last_row - 1,), everything, wl, last_row))
        finish_row(last_row, everything, last)
        if send:
            for g in groups:
                for h in halves:
                    fwd_copy(k, g, h).start()

    def take_last_u(k):
        for g in groups:
            for h in halves:
                back_copy(k, g, h).wait_recv()
        store_sub(st, (last_row,), everything, ft, (last_row,),
                  product(rr, (k,), everything, wu, last_row))

    def turn_out(row):
        for n in range(tiles):
            out[row, nds(n), :] = st[row, :, nds(n)].T

    def sweep(k, last):
        @pl.when(first)
        def _():
            for n in range(tiles):
                tb[:, nds(n)] = st[0, :, nds(n)].astype(BF16)
            finish_row(0, everything, last)

        @pl.when(pos == mid)
        def _():
            first_row(k, by_group, last)
            if last:
                turn_out(0)

        @pl.when(has_left & (pos != mid))
        def _():
            first_row(k, at_once, last)

        for row in range(1, last_row):
            store_t(everything, st, (row,), product(xt, (row - 1,), everything, wl, row))
            if row > 1 and not last:
                u_product(row - 2, range(tiles // 2))
            finish_row(row, everything, last)
            if row > 1 and not last:
                u_product(row - 2, range(tiles // 2, tiles))

        @pl.when(has_right & (k > 0))
        def _():
            for g in groups:
                for h in halves:
                    fwd_copy(k - 1, g, h).wait_send()

        @pl.when((pos == mid - 1) & (k > 0))
        def _():
            store_sub(tmp, (), everything, ft, (last_row,),
                      product(xt, (last_row - 1,), everything, wl, last_row))
            for r, members in by_group:
                for h in halves:
                    for g in members:
                        back_copy(k, g, h).wait_recv()
                store_t(r, tmp, (), product(rr, (k,), r, wu, last_row))

                def send(h):
                    for g in members:
                        fwd_copy(k, g, h).start()

                finish_and_send(last_row, r, last, send)
            if last:
                turn_out(last_row)

        @pl.when(has_right & (pos != mid - 1) & (k > 0))
        def _():
            take_last_u(k)

        @pl.when(has_right & ((pos != mid - 1) | (k == 0)))
        def _():
            last_row_plain(k, last, True)

        @pl.when(jnp.logical_not(has_right))
        def _():
            last_row_plain(k, last, False)

        if not last:
            for row in range(last_row - 2, last_row):
                u_product(row)

    def mid_sweep(k, carry):
        sweep(k, False)
        return carry

    lax.fori_loop(first.astype(jnp.int32), SWEEPS - 1, mid_sweep, 0)
    sweep(SWEEPS - 1, True)

    @pl.when(has_right)
    def _():
        for g in groups:
            for h in halves:
                fwd_copy(SWEEPS - 1, g, h).wait_send()


def solution(mesh):
    chain_len = mesh.shape["row"]
    mat_spec = P(("batch", "row"), None, None)
    vec_spec = P(("batch", "row"), None, "col")

    def device_fn(d_inv, l_blk, u_blk, rhs_blk, x_init):
        rows, size, cols = rhs_blk.shape
        any_spec = pl.BlockSpec(memory_space=pl.ANY)
        dma = pltpu.SemaphoreType.DMA
        return pl.pallas_call(
            lambda *refs: kernel(chain_len, *refs),
            out_shape=pltpu.VMEM(rhs_blk.shape, F32),
            in_specs=[any_spec] * 5,
            out_specs=pl.BlockSpec(memory_space=pltpu.VMEM),
            scratch_shapes=[
                pltpu.VMEM((rows, size, size), BF16),
                pltpu.VMEM((rows, size, size), BF16),
                pltpu.VMEM((rows, size, size), BF16),
                pltpu.VMEM((rows, size, cols), F32),
                pltpu.VMEM((rows, size, cols), F32),
                pltpu.VMEM((rows, cols, size), F32),
                pltpu.VMEM((rows, cols, size), F32),
                pltpu.VMEM((cols, size), F32),
                pltpu.VMEM((cols, size), BF16),
                pltpu.VMEM((rows + 2, cols, size), BF16),
                pltpu.VMEM((SWEEPS, cols, size), BF16),
                pltpu.VMEM((SWEEPS, cols, size), BF16),
                pltpu.VMEM((TILE, TILE), BF16),
                dma((rows,)), dma((rows,)), dma((rows,)), dma((rows,)), dma((rows,)),
                *[dma((SWEEPS, len(GROUPS), HALVES))] * 4,
            ],
            compiler_params=pltpu.CompilerParams(
                collective_id=0, has_side_effects=True,
                vmem_limit_bytes=57 * 1024 * 1024),
        )(d_inv, l_blk, u_blk, rhs_blk, x_init)

    return jax.shard_map(device_fn, mesh=mesh, in_specs=(mat_spec, mat_spec, mat_spec, vec_spec, vec_spec),
                         out_specs=vec_spec, check_vma=False)
```
